32 devices in a mesh: row: 8 (over z, x), col: 4 (over y, core).
Axes of the slice: x: 2, y: 2, z: 4, core: 2. Of those that a mesh axis runs over, the one named last changes fastest.
Arguments:
- features: bfloat16 [4096, 512], P(('row', 'col')), may hold values from -6 to 6
- adjacency: bfloat16 [4096, 4096], P('row', 'col'), may hold values from -0.546875 to 0.546875
- block_pattern: int32 [64, 64], P('row', 'col'), may hold values from 0 to 1, as said below
- weight_in: bfloat16 [512, 256], replicated, may hold values from -0.25 to 0.25
- bias_in: float32 [256], replicated, may hold values from -3 to 3
- weight_out: bfloat16 [256, 256], replicated, may hold values from -0.75 to 0.75
- bias_out: float32 [256], replicated, may hold values from -3 to 3
Outputs:
- embeddings: bfloat16 [4096, 256], P(('row', 'col'))
The draws below stay inside these ranges and needn't reach their ends.
Inputs may be any that keep to these rules, and one draw needn't show every extreme that they name: `block_pattern`: in each aligned tile of 8 rows by 16 columns, at most half of the entries are 1; some tile has exactly half.
All inputs are finite; a program needn't handle non-finite values.
Results may differ from the reference program's by a relative error of at most 0.015.
Values may be sent and summed in bfloat16 or wider, within the bound.
A program may use at most 64 MiB of HBM per device.

```python
import math
import jax
import jax.numpy as jnp
from jax import lax

FIN = 512
HID = 256
BLK = 64
NODE_DEV = 128
NODES = 4096
TILE_ROWS = 512
N_ROW = 8
N_COL = 4


def draw_adjacency(key, part):
    node_count = NODE_DEV * N_ROW * N_COL
    first_key, second_key, third_key = jax.random.split(jax.random.fold_in(key, 23), 3)
    values = jax.random.truncated_normal(first_key, -4.0, 4.0, (node_count, node_count), jnp.float32)
    row_scale = jnp.exp(0.5 * jax.random.uniform(second_key, (node_count, 1), jnp.float32, 0.0, math.log(10.0)))
    col_scale = jnp.exp(0.5 * jax.random.uniform(third_key, (1, node_count), jnp.float32, 0.0, math.log(10.0)))
    column_device = (jnp.arange(node_count, dtype=jnp.int32) // (NODE_DEV * N_ROW)).astype(jnp.float32)
    col_ramp = jnp.exp(0.5 * math.log(3.0) * column_device / max(N_COL - 1, 1))
    scaled_values = values * row_scale * col_scale * col_ramp[None, :] * (0.5 / math.sqrt(node_count))
    return scaled_values.astype(jnp.bfloat16)


def draw_block_pattern(key, part):
    row_blocks = NODE_DEV * N_COL // BLK
    col_blocks = NODE_DEV * N_ROW // BLK
    per_tile = row_blocks * col_blocks
    most_blocks = per_tile // 2
    tile_count = N_ROW * N_COL
    first_key, second_key, third_key = jax.random.split(jax.random.fold_in(key, 11), 3)
    spread = jax.random.randint(first_key, (tile_count,), 0, most_blocks + 1)
    counts = jnp.maximum(jnp.maximum(1, most_blocks // 8), spread * spread // max(most_blocks, 1))
    chosen = jax.random.randint(second_key, (), 0, tile_count)
    counts = jnp.where(jnp.arange(tile_count, dtype=jnp.int32) == chosen, most_blocks, counts)
    scores = jax.random.randint(third_key, (tile_count, per_tile), 0, (1 << 30) // per_tile)
    scores = scores * per_tile + jnp.arange(per_tile, dtype=jnp.int32)[None, :]
    rank_of = jnp.argsort(jnp.argsort(scores, axis=1), axis=1)
    pattern = (rank_of < counts[:, None]).astype(jnp.int32)
    pattern = pattern.reshape(N_ROW, N_COL, row_blocks, col_blocks).transpose(0, 2, 1, 3)
    return pattern.reshape(N_ROW * row_blocks, N_COL * col_blocks)


def levels(key, extent, shards, least, largest):
    def one(position, shards_of):
        draws = jax.random.uniform(jax.random.fold_in(jax.random.fold_in(key, 6), position), (shards_of,), jnp.float32, least / len(shards), largest / len(shards))
        return jnp.repeat(jnp.exp(draws), extent[position] // shards_of).reshape((-1,) + (1,) * (len(extent) - position - 1))

    gain = one(*shards[0])
    for cut in shards[1:]:
        gain = gain * one(*cut)
    return gain


def normal_values(rng, dims, scale, bound, cuts=(), held_as=jnp.bfloat16):
    entries = jax.random.normal(rng, dims, jnp.float32) * scale
    if len(cuts) > 0:
        entries = levels(rng, dims, cuts, -0.22, 0.18) * entries
    return jnp.clip(entries, min=-bound, max=bound).astype(held_as)


def setup_inputs(seed: int = 0) -> dict:
    splits = jax.random.split(jax.random.key(seed), 8)
    return {
        "features": normal_values(splits[0], (NODES, FIN), 1.0, 6.0, ((0, 32),)),
        "adjacency": draw_adjacency(jax.random.fold_in(splits[7], 71), 0),
        "block_pattern": draw_block_pattern(jax.random.fold_in(splits[7], 71), 0),
        "weight_in": normal_values(splits[3], (FIN, HID), FIN ** -0.5, 0.25),
        "bias_in": normal_values(splits[4], (HID,), 0.5, 3.0, (), jnp.float32),
        "weight_out": normal_values(splits[5], (HID, HID), (HID // 4) ** -0.5, 0.75),
        "bias_out": normal_values(splits[6], (HID,), 0.5, 3.0, (), jnp.float32),
    }


def stored_order(values):
    feat_width = values.shape[1]
    grid = values.reshape(N_ROW, N_COL, NODE_DEV, feat_width)
    return grid.transpose(1, 0, 2, 3).reshape(NODES, feat_width)

def masked_rows(adjacency, block_pattern, block_index):
    adj_rows = lax.dynamic_slice_in_dim(adjacency, block_index * TILE_ROWS, TILE_ROWS, 0).astype(jnp.float32)
    block_marks = lax.dynamic_slice_in_dim(block_pattern, block_index * (TILE_ROWS // BLK), TILE_ROWS // BLK, 0)
    present = jnp.repeat(jnp.repeat((block_marks == 1).astype(jnp.float32), BLK, axis=0), BLK, axis=1)
    return adj_rows * present

def aggregate(adjacency, block_pattern, scaled):
    source = stored_order(scaled).astype(jnp.float32)

    def one_block(block_index):
        return jnp.dot(masked_rows(adjacency, block_pattern, block_index), source, precision=lax.Precision.HIGHEST)
    return lax.map(one_block, jnp.arange(N_ROW, dtype=jnp.int32)).reshape(NODES, scaled.shape[1])

def reference(features, adjacency, block_pattern, weight_in, bias_in, weight_out, bias_out):

    def block_squares(block_index):
        return lax.optimization_barrier(jnp.sum(jnp.square(masked_rows(adjacency, block_pattern, block_index)), axis=1))
    squares = lax.map(block_squares, jnp.arange(N_ROW, dtype=jnp.int32)).reshape(NODES)
    inv_root = lax.rsqrt(1.0 + squares)[:, None]
    projected = jnp.dot(features, weight_in, preferred_element_type=jnp.float32)
    scaled = (inv_root * projected).astype(jnp.bfloat16)
    summed = aggregate(adjacency, block_pattern, scaled) + scaled.astype(jnp.float32)
    hidden = jax.nn.relu(inv_root * summed + bias_in[None, :]).astype(jnp.bfloat16)
    projected_out = jnp.dot(hidden, weight_out, preferred_element_type=jnp.float32)
    scaled_out = (inv_root * projected_out).astype(jnp.bfloat16)
    summed_out = aggregate(adjacency, block_pattern, scaled_out) + scaled_out.astype(jnp.float32)
    return (inv_root * summed_out + bias_out[None, :]).astype(jnp.bfloat16)
```

```python
import functools

import jax
import jax.numpy as jnp
from jax import lax
from jax.experimental import pallas as pl
from jax.experimental.pallas import tpu as pltpu
from jax.sharding import PartitionSpec as P

MESH = pl.DeviceIdType.MESH
F32 = jnp.float32
BF16 = jnp.bfloat16
UNROLL = 16


def steps(count, body):
    if count <= UNROLL:
        for step in range(count):
            body(step)
    else:
        pl.loop(0, count)(body)


def kernel(
    n_row, n_col,
    features, adjacency, pattern, weight_in, bias_in, weight_out, bias_out, out,
    masked, squares, total, rows_in, rows_out, scaled, part_in, part_out, got_in, got_out,
    degree_send, degree_got, roots, root_tile,
    send_rows, recv_rows, send_part, recv_part, send_degree, recv_degree, send_root, recv_root,
):
    row, col = lax.axis_index("row"), lax.axis_index("col")
    own, width = rows_in.shape[1], rows_in.shape[2]
    row_blocks = pattern.shape[0]
    side = adjacency.shape[0] // row_blocks

    def row_peer(step):
        return lax.rem(row + step, n_row)

    def col_peer(step):
        return lax.rem(col + step, n_col)

    barrier = pltpu.get_barrier_semaphore()

    def greet_row(step):
        pl.semaphore_signal(barrier, inc=1, device_id=(row_peer(step + 1), col), device_id_type=MESH)

    def greet_col(step):
        pl.semaphore_signal(barrier, inc=1, device_id=(row, col_peer(step + 1)), device_id_type=MESH)

    steps(n_row - 1, greet_row)
    steps(n_col - 1, greet_col)

    def rows_copy(buffer, layer, step):
        return pltpu.make_async_remote_copy(
            src_ref=buffer.at[row], dst_ref=buffer.at[row],
            send_sem=send_rows.at[layer, step], recv_sem=recv_rows.at[layer, step],
            device_id=(row_peer(step), col), device_id_type=MESH,
        )

    def part_copy(source, landing, layer, step):
        return pltpu.make_async_remote_copy(
            src_ref=source.at[col_peer(step)], dst_ref=landing.at[step],
            send_sem=send_part.at[layer, step], recv_sem=recv_part.at[layer, step],
            device_id=(row, col_peer(step)), device_id_type=MESH,
        )

    def degree_copy(step):
        return pltpu.make_async_remote_copy(
            src_ref=degree_send.at[col_peer(step)], dst_ref=degree_got.at[step],
            send_sem=send_degree.at[step], recv_sem=recv_degree.at[step],
            device_id=(row, col_peer(step)), device_id_type=MESH,
        )

    def root_copy(step):
        return pltpu.make_async_remote_copy(
            src_ref=roots.at[row], dst_ref=roots.at[row],
            send_sem=send_root.at[step], recv_sem=recv_root.at[step],
            device_id=(row_peer(step), col), device_id_type=MESH,
        )

    projected = jnp.dot(features[...], weight_in[...], preferred_element_type=F32)
    rows_in[row] = projected.astype(BF16)
    pl.semaphore_wait(barrier, n_row + n_col - 2)
    steps(n_row - 1, lambda step: rows_copy(rows_in, 0, step + 1).start())

    col_blocks = pattern.shape[1]
    lane = lax.broadcasted_iota(jnp.int32, (col_blocks, col_blocks * side), 1)
    block = lax.broadcasted_iota(jnp.int32, (col_blocks, col_blocks * side), 0)
    spread = jnp.where(lane // side == block, 1.0, 0.0).astype(BF16)
    marks = jnp.where(pattern[...] == 1, 1.0, 0.0).astype(BF16)
    wide = jnp.dot(marks, spread, preferred_element_type=F32)
    for owner in range(n_row):
        root_tile[owner] = wide[:, owner * own:(owner + 1) * own]
    squares[...] = jnp.zeros_like(squares)

    def mask_slab(owner):
        start = owner * own if isinstance(owner, int) else pl.multiple_of(owner * own, own)
        for r in range(row_blocks):
            rows = pl.ds(r * side, side)
            mark = root_tile[owner, r:r + 1, :]
            piece = adjacency[rows, pl.ds(start, own)].astype(F32) * mark
            squares[rows, :] += piece * piece
            masked[owner, rows, :] = piece.astype(BF16)

    steps(n_row, mask_slab)
    ones = jnp.ones((8, own), BF16)
    high = squares[...].astype(BF16)
    low = (squares[...] - high.astype(F32)).astype(BF16)
    contract = (((1,), (1,)), ((), ()))
    sums = lax.dot_general(ones, high, contract, preferred_element_type=F32)
    sums = sums + lax.dot_general(ones, low, contract, preferred_element_type=F32)
    for peer in range(n_col):
        degree_send[peer] = sums[:, peer * own:(peer + 1) * own]
    steps(n_col - 1, lambda step: degree_copy(step + 1).start())
    degree_got[0] = degree_send[col]
    for step in range(1, n_col):
        degree_copy(step).wait_recv()
    degree = 1.0 + degree_got[0]
    for step in range(1, n_col):
        degree = degree + degree_got[step]
    roots[row] = lax.rsqrt(degree)
    steps(n_row - 1, lambda step: root_copy(step + 1).start())

    def root_column(owner):
        return jnp.broadcast_to(roots[owner, 0:1, :], (own, own)).T

    def widen(column):
        return jnp.concatenate([column] * (width // own), axis=1)

    inv_root = widen(root_column(row))
    own_in = inv_root * projected

    def layer(buffer, index, first):
        def add(step):
            owner = row_peer(n_row - step)
            if not (isinstance(step, int) and step == 0):
                rows_copy(buffer, index, step).wait_recv()
                if first:
                    root_copy(step).wait_recv()
            values = buffer[owner]
            if first:
                values = (widen(root_column(owner)) * values.astype(F32)).astype(BF16)
            product = jnp.dot(masked[owner], values, preferred_element_type=F32)
            if isinstance(step, int) and step == 0:
                total[...] = product
            else:
                total[...] += product

        add(0)
        if n_row <= UNROLL:
            for step in range(1, n_row):
                add(step)
        else:
            pl.loop(1, n_row)(add)

    def collect(source, landing, index):
        for step in list(range(1, n_col)):
            peer = col_peer(step)
            source[peer] = total[pl.ds(pl.multiple_of(peer * own, own), own), :].astype(BF16)
            part_copy(source, landing, index, step).start()
        mine = total[pl.ds(pl.multiple_of(col * own, own), own), :]
        for step in range(1, n_col):
            part_copy(source, landing, index, step).wait_recv()
            mine = mine + landing[step].astype(F32)
        return mine

    layer(rows_in, 0, True)
    summed = collect(part_in, got_in, 0) + own_in
    hidden = jnp.maximum(inv_root * summed + bias_in[...], 0.0).astype(BF16)
    scaled_out = inv_root * jnp.dot(hidden, weight_out[...], preferred_element_type=F32)
    rows_out[row] = scaled_out.astype(BF16)
    steps(n_row - 1, lambda step: rows_copy(rows_out, 1, step + 1).start())
    layer(rows_out, 1, False)
    summed_out = collect(part_out, got_out, 1) + scaled_out
    out[...] = (inv_root * summed_out + bias_out[...]).astype(BF16)

    def drain_rows(step):
        rows_copy(rows_in, 0, step + 1).wait_send()
        rows_copy(rows_out, 1, step + 1).wait_send()
        root_copy(step + 1).wait_send()

    def drain_cols(step):
        part_copy(part_in, got_in, 0, step + 1).wait_send()
        part_copy(part_out, got_out, 1, step + 1).wait_send()
        degree_copy(step + 1).wait_send()

    steps(n_row - 1, drain_rows)
    steps(n_col - 1, drain_cols)


def body(n_row, n_col, features, adjacency, pattern, weight_in, bias_in, weight_out, bias_out):
    own, width = features.shape[0], weight_out.shape[1]
    height = adjacency.shape[0]
    dma = pltpu.SemaphoreType.DMA
    vmem = pl.BlockSpec(memory_space=pltpu.VMEM)
    return pl.pallas_call(
        functools.partial(kernel, n_row, n_col),
        out_shape=jax.ShapeDtypeStruct((own, width), BF16),
        in_specs=[vmem] * 7,
        out_specs=vmem,
        scratch_shapes=[
            pltpu.VMEM((n_row, height, own), BF16),
            pltpu.VMEM((height, own), F32),
            pltpu.VMEM((height, width), F32),
            pltpu.VMEM((n_row, own, width), BF16),
            pltpu.VMEM((n_row, own, width), BF16),
            pltpu.VMEM((own, width), BF16),
            pltpu.VMEM((n_col, own, width), BF16),
            pltpu.VMEM((n_col, own, width), BF16),
            pltpu.VMEM((n_col, own, width), BF16),
            pltpu.VMEM((n_col, own, width), BF16),
            pltpu.VMEM((n_col, 8, own), F32),
            pltpu.VMEM((n_col, 8, own), F32),
            pltpu.VMEM((n_row, 8, own), F32),
            pltpu.VMEM((n_row, pattern.shape[0], own), F32),
            dma((2, n_row)), dma((2, n_row)), dma((2, n_col)), dma((2, n_col)),
            dma((n_col,)), dma((n_col,)), dma((n_row,)), dma((n_row,)),
        ],
        compiler_params=pltpu.CompilerParams(
            collective_id=0, has_side_effects=True, vmem_limit_bytes=60 * 1024 * 1024
        ),
    )(features, adjacency, pattern, weight_in, bias_in[None, :], weight_out, bias_out[None, :])


def solution(mesh):
    placed = (P(("row", "col"), None), P("row", "col"), P("row", "col"), P(), P(), P(), P())
    return jax.shard_map(
        functools.partial(body, mesh.shape["row"], mesh.shape["col"]),
        mesh=mesh, in_specs=placed, out_specs=P(("row", "col"), None), check_vma=False,
    )
```

```python
import functools

import jax
import jax.numpy as jnp
from jax import lax
from jax.experimental import pallas as pl
from jax.experimental.pallas import tpu as pltpu
from jax.sharding import PartitionSpec as P

MESH = pl.DeviceIdType.MESH
F32 = jnp.float32
BF16 = jnp.bfloat16


def kernel(
    n_lo, n_col,
    features_in, adjacency_in, pattern_in, weight_one_in, bias_one_in, weight_two_in, bias_two_in, out,
    features, adjacency, pattern, weight_in, bias_in, weight_out, bias_out,
    masked, squares, marked, total, rows_in, rows_out, part_in, part_out, got_in, got_out,
    degree_send, degree_got, roots, load,
    send_hi, recv_hi, send_lo, recv_lo, send_part, recv_part,
    send_degree, recv_degree, send_root, recv_root,
):
    row, col = lax.axis_index("row"), lax.axis_index("col")
    halves, n_row, own, width = rows_in.shape
    n_hi = n_row // n_lo
    hi, lo = row // n_lo, row % n_lo
    row_blocks, col_blocks = pattern.shape
    side = adjacency.shape[0] // row_blocks

    def hi_peer(step):
        return lax.rem(hi + step, n_hi) * n_lo + lo

    def lo_peer(step):
        return hi * n_lo + lax.rem(lo + step, n_lo)

    def col_peer(step):
        return lax.rem(col + step, n_col)

    barrier = pltpu.get_barrier_semaphore()

    def greet(target):
        pl.semaphore_signal(barrier, inc=1, device_id=target, device_id_type=MESH)

    for step in range(1, n_hi):
        greet((hi_peer(step), col))
    for step in range(1, n_lo):
        greet((lo_peer(step), col))
    for step in range(1, n_col):
        greet((row, col_peer(step)))

    pairs = [
        (features_in, features), (weight_one_in, weight_in), (pattern_in, pattern),
        (adjacency_in, adjacency), (bias_one_in, bias_in), (weight_two_in, weight_out),
        (bias_two_in, bias_out),
    ]
    loads = [pltpu.make_async_copy(a, b, load.at[i]) for i, (a, b) in enumerate(pairs)]
    for copy in loads:
        copy.start()

    def hi_copy(buffer, layer, half, step, owner):
        return pltpu.make_async_remote_copy(
            src_ref=buffer.at[half, owner], dst_ref=buffer.at[half, owner],
            send_sem=send_hi.at[layer, half, step], recv_sem=recv_hi.at[layer, half, step],
            device_id=(hi_peer(step), col), device_id_type=MESH,
        )

    def lo_copy(buffer, layer, half, back, step, owner):
        return pltpu.make_async_remote_copy(
            src_ref=buffer.at[half, owner], dst_ref=buffer.at[half, owner],
            send_sem=send_lo.at[layer, half, back, step], recv_sem=recv_lo.at[layer, half, back, step],
            device_id=(lo_peer(step), col), device_id_type=MESH,
        )

    def root_hi(step, owner):
        return pltpu.make_async_remote_copy(
            src_ref=roots.at[owner], dst_ref=roots.at[owner],
            send_sem=send_root.at[step, 0], recv_sem=recv_root.at[step, 0],
            device_id=(hi_peer(step), col), device_id_type=MESH,
        )

    def root_lo(back, step, owner):
        return pltpu.make_async_remote_copy(
            src_ref=roots.at[owner], dst_ref=roots.at[owner],
            send_sem=send_root.at[back, step], recv_sem=recv_root.at[back, step],
            device_id=(lo_peer(step), col), device_id_type=MESH,
        )

    def part_copy(source, landing, layer, half, step):
        return pltpu.make_async_remote_copy(
            src_ref=source.at[half, step], dst_ref=landing.at[half, step],
            send_sem=send_part.at[layer, half, step], recv_sem=recv_part.at[layer, half, step],
            device_id=(row, col_peer(step)), device_id_type=MESH,
        )

    def degree_copy(step):
        return pltpu.make_async_remote_copy(
            src_ref=degree_send.at[col_peer(step)], dst_ref=degree_got.at[step],
            send_sem=send_degree.at[step], recv_sem=recv_degree.at[step],
            device_id=(row, col_peer(step)), device_id_type=MESH,
        )

    def holder(back):
        return lax.rem(hi + n_hi - back, n_hi) * n_lo + lo

    def send_own(buffer, layer):
        for half in range(halves):
            for step in range(1, n_hi):
                hi_copy(buffer, layer, half, step, row).start()
            for step in range(1, n_lo):
                lo_copy(buffer, layer, half, 0, step, row).start()

    def pass_on(buffer, layer, half):
        for back in range(1, n_hi):
            hi_copy(buffer, layer, half, back, row).wait_recv()
            for step in range(1, n_lo):
                lo_copy(buffer, layer, half, back, step, holder(back)).start()

    loads[0].wait()
    loads[1].wait()
    projected = jnp.dot(features[...], weight_in[...], preferred_element_type=F32)
    for half in range(halves):
        rows_in[half, row] = projected[:, half * width:(half + 1) * width].astype(BF16)
    loads[2].wait()
    loads[3].wait()

    lane = lax.broadcasted_iota(jnp.int32, (col_blocks, col_blocks * side), 1)
    block = lax.broadcasted_iota(jnp.int32, (col_blocks, col_blocks * side), 0)
    spread = jnp.where(lane // side == block, 1.0, 0.0).astype(BF16)
    marks = jnp.where(pattern[...] == 1, 1.0, 0.0).astype(BF16)
    wide = jnp.dot(marks, spread, preferred_element_type=F32)
    for owner in range(n_row):
        marked[owner] = wide[:, owner * own:(owner + 1) * own]

    def mask_rows(r):
        start = r * side if isinstance(r, int) else pl.multiple_of(r * side, side)
        rows = pl.ds(start, side)
        square = jnp.zeros((side, own), F32)
        for owner in range(n_row):
            mark = marked[owner, pl.ds(r, 1), :]
            piece = adjacency[rows, owner * own:(owner + 1) * own].astype(F32) * mark
            square = square + piece * piece
            masked[owner, rows, :] = piece.astype(BF16)
        squares[rows, :] = square

    if n_row * row_blocks <= 64:
        for r in range(row_blocks):
            mask_rows(r)
    else:
        pl.loop(0, row_blocks)(mask_rows)

    pl.semaphore_wait(barrier, n_hi + n_lo + n_col - 3)
    send_own(rows_in, 0)

    ones = jnp.ones((8, own), BF16)
    high = squares[...].astype(BF16)
    low = (squares[...] - high.astype(F32)).astype(BF16)
    contract = (((1,), (1,)), ((), ()))
    sums = lax.dot_general(ones, high, contract, preferred_element_type=F32)
    sums = sums + lax.dot_general(ones, low, contract, preferred_element_type=F32)
    for peer in range(n_col):
        degree_send[peer] = sums[:, peer * own:(peer + 1) * own]
    for step in range(1, n_col):
        degree_copy(step).start()
    degree = 1.0 + degree_send[col]
    for step in range(1, n_col):
        degree_copy(step).wait_recv()
        degree = degree + degree_got[step]
    roots[row] = lax.rsqrt(degree)
    for step in range(1, n_hi):
        root_hi(step, row).start()
    for step in range(1, n_lo):
        root_lo(0, step, row).start()

    def root_column(owner):
        return jnp.broadcast_to(roots[owner, 0:1, :], (own, own)).T

    inv_root = root_column(row)

    def layer(buffer, index):
        def add(half, owner, fresh=False):
            values = buffer[half, owner]
            if index == 0:
                values = (root_column(owner) * values.astype(F32)).astype(BF16)
            product = jnp.dot(masked[owner], values, preferred_element_type=F32)
            if fresh:
                total[half] = product
            else:
                total[half] += product

        for half in range(halves):
            add(half, row, True)
        for half in range(halves):
            pass_on(buffer, index, half)
            if index == 0 and half == 0:
                for back in range(1, n_hi):
                    root_hi(back, row).wait_recv()
                    for step in range(1, n_lo):
                        root_lo(back, step, holder(back)).start()
        for half in range(halves):
            for back in range(1, n_hi):
                add(half, holder(back))
            for back in range(n_hi):
                def arrived(step):
                    owner = lax.rem(hi + n_hi - back, n_hi) * n_lo + lax.rem(lo + n_lo - step, n_lo)
                    lo_copy(buffer, index, half, back, step, row).wait_recv()
                    if index == 0 and half == 0:
                        root_lo(back, step, row).wait_recv()
                    add(half, owner)

                if n_lo <= 4:
                    for step in range(1, n_lo):
                        arrived(step)
                else:
                    pl.loop(1, n_lo)(arrived)
            yield half

    def collect(buffer, source, landing, index):
        for half in layer(buffer, index):
            for step in range(1, n_col):
                rows = pl.ds(pl.multiple_of(col_peer(step) * own, own), own)
                source[half, step] = total[half, rows, :].astype(BF16)
                part_copy(source, landing, index, half, step).start()
        sums = []
        for half in range(halves):
            mine = total[half, pl.ds(pl.multiple_of(col * own, own), own), :]
            for step in range(1, n_col):
                part_copy(source, landing, index, half, step).wait_recv()
                mine = mine + landing[half, step].astype(F32)
            sums.append(mine)
        return sums

    def cut(value, half):
        return value[:, half * width:(half + 1) * width]

    loads[4].wait()
    loads[5].wait()
    loads[6].wait()
    summed = collect(rows_in, part_in, got_in, 0)
    projected_out = jnp.zeros((own, halves * width), F32)
    for half in range(halves):
        hidden = inv_root * (summed[half] + inv_root * cut(projected, half)) + cut(bias_in[...], half)
        hidden = jnp.maximum(hidden, 0.0).astype(BF16)
        projected_out += jnp.dot(
            hidden, weight_out[half * width:(half + 1) * width, :], preferred_element_type=F32
        )
    scaled_out = [inv_root * cut(projected_out, half) for half in range(halves)]
    for half in range(halves):
        rows_out[half, row] = scaled_out[half].astype(BF16)
    send_own(rows_out, 1)
    summed_out = collect(rows_out, part_out, got_out, 1)
    for half in range(halves):
        final = inv_root * (summed_out[half] + scaled_out[half]) + cut(bias_out[...], half)
        out[:, half * width:(half + 1) * width] = final.astype(BF16)

    for layer_index, (buffer, source, landing) in enumerate(
        ((rows_in, part_in, got_in), (rows_out, part_out, got_out))
    ):
        for half in range(halves):
            for step in range(1, n_hi):
                hi_copy(buffer, layer_index, half, step, row).wait_send()
            for back in range(n_hi):
                for step in range(1, n_lo):
                    lo_copy(buffer, layer_index, half, back, step, row).wait_send()
            for step in range(1, n_col):
                part_copy(source, landing, layer_index, half, step).wait_send()
    for step in range(1, n_col):
        degree_copy(step).wait_send()
    for back in range(1, n_hi):
        root_hi(back, row).wait_send()
    for back in range(n_hi):
        for step in range(1, n_lo):
            root_lo(back, step, row).wait_send()


def body(n_row, n_lo, n_col, features, adjacency, pattern, weight_in, bias_in, weight_out, bias_out):
    own, width = features.shape[0], weight_out.shape[1]
    height = adjacency.shape[0]
    half = own
    halves = width // half
    n_hi = n_row // n_lo
    dma = pltpu.SemaphoreType.DMA
    args = (features, adjacency, pattern, weight_in, bias_in[None, :], weight_out, bias_out[None, :])
    return pl.pallas_call(
        functools.partial(kernel, n_lo, n_col),
        out_shape=jax.ShapeDtypeStruct((own, width), BF16),
        in_specs=[pl.BlockSpec(memory_space=pl.ANY)] * len(args),
        out_specs=pl.BlockSpec(memory_space=pltpu.VMEM),
        scratch_shapes=[pltpu.VMEM(arg.shape, arg.dtype) for arg in args] + [
            pltpu.VMEM((n_row, height, own), BF16),
            pltpu.VMEM((height, own), F32),
            pltpu.VMEM((n_row, pattern.shape[0], own), F32),
            pltpu.VMEM((halves, height, half), F32),
            pltpu.VMEM((halves, n_row, own, half), BF16),
            pltpu.VMEM((halves, n_row, own, half), BF16),
            pltpu.VMEM((halves, n_col, own, half), BF16),
            pltpu.VMEM((halves, n_col, own, half), BF16),
            pltpu.VMEM((halves, n_col, own, half), BF16),
            pltpu.VMEM((halves, n_col, own, half), BF16),
            pltpu.VMEM((n_col, 8, own), F32),
            pltpu.VMEM((n_col, 8, own), F32),
            pltpu.VMEM((n_row, 8, own), F32),
            dma((len(args),)),
            dma((2, halves, n_hi)), dma((2, halves, n_hi)),
            dma((2, halves, n_hi, n_lo)), dma((2, halves, n_hi, n_lo)),
            dma((2, halves, n_col)), dma((2, halves, n_col)),
            dma((n_col,)), dma((n_col,)), dma((n_hi, n_lo)), dma((n_hi, n_lo)),
        ],
        compiler_params=pltpu.CompilerParams(
            collective_id=0, has_side_effects=True, vmem_limit_bytes=60 * 1024 * 1024
        ),
    )(*args)


def fast_extent(mesh):
    count = mesh.shape["row"]
    places = [tuple(getattr(device, "coords", None) or ()) for device in mesh.devices[:, 0]]
    if not places[0]:
        return 2 if count % 2 == 0 else 1
    moved = [[a != b for a, b in zip(place, places[0])] for place in places]
    extent = 2
    while extent < count and moved[extent] == moved[1]:
        extent += 1
    return extent


def solution(mesh):
    placed = (P(("row", "col"), None), P("row", "col"), P("row", "col"), P(), P(), P(), P())
    return jax.shard_map(
        functools.partial(body, mesh.shape["row"], fast_extent(mesh), mesh.shape["col"]),
        mesh=mesh, in_specs=placed, out_specs=P(("row", "col"), None), check_vma=False,
    )
```
